32 devices in a mesh: seq: 8 (over z, x), mp: 4 (over y, core).
Axes of the slice: x: 2, y: 2, z: 4, core: 2. Of those that a mesh axis runs over, the one named last changes fastest.
Arguments:
- tokens: bfloat16 [2048, 2560], P('seq'), may hold values from -6 to 6
- w_in: bfloat16 [2560, 4096], P('seq', 'mp'), may hold values from -0.125 to 0.125
- b_in: float32 [2048, 128], P('seq'), may hold values from -0.6 to 0.6
- c_in: float32 [2048, 128], P('seq'), may hold values from -0.6 to 0.6
- dt: float32 [64, 2048], P('mp', 'seq'), may hold values from 0.05 to 0.2
- log_rate: float32 [64], P('mp'), as said below
- cot: bfloat16 [2048, 4096], P('seq', 'mp'), may hold values from -6 to 6
Outputs:
- mixed: bfloat16 [2048, 4096], P('seq', 'mp')
- direction: float32 [2560, 4096], P('seq', 'mp')
- perturbed: float32 [2560, 4096], P('seq', 'mp')
- perturbed_rate: float32 [64], P('mp')
The draws below stay inside these ranges and needn't reach their ends.
Inputs may be any that keep to these rules, and one draw needn't show every extreme that they name: exp(log_rate) lies between 1 / 2048 and 0.5; some heads decay within some tens of tokens, others keep their state over the whole sequence.
All inputs are finite; a program needn't handle non-finite values.
Results may differ from the reference program's by a relative error of at most 0.0049.
Values may be sent and summed in bfloat16 or wider, within the bound.
A program may use at most 128 MiB of HBM per device.

```python
import math
import jax
import jax.numpy as jnp
from jax import lax

D = 2560
H = 64
P_SIZE = 64
N = 128
Q = 256
TOKENS = 2048


def draw_log_rate(key, part):
    first, second, third = jax.random.split(key, 3)
    order = jax.random.permutation(first, H)
    quick = order < H // 2
    slow_rate = jnp.exp(jax.random.uniform(second, (H,), jnp.float32, math.log(1.0 / TOKENS), math.log(10.0 / TOKENS)))
    quick_rate = jnp.exp(jax.random.uniform(third, (H,), jnp.float32, math.log(0.15), math.log(0.5)))
    return jnp.log(jnp.where(quick, quick_rate, slow_rate)).astype(jnp.float32)


def shard_levels(key, shape, pieces, smallest, largest):
    level, own = 1.0, jax.random.fold_in(key, 6)
    for position, shards_of in pieces:
        draws = jnp.exp(jax.random.uniform(jax.random.fold_in(own, position), (shards_of,), jnp.float32, smallest / len(pieces), largest / len(pieces)))
        level = level * jnp.repeat(draws, shape[position] // shards_of).reshape([-1 if axis == position else 1 for axis in range(len(shape))])
    return level


def centred(stream_key, extent, scale, most, shards=(), dtype=jnp.bfloat16):
    gain = shard_levels(stream_key, extent, shards, -0.22, 0.18) if shards else 1.0
    result = jax.random.normal(stream_key, extent, jnp.float32) * scale * gain
    return jnp.minimum(jnp.maximum(result, -most), most).astype(dtype)


def setup_inputs(seed: int = 0) -> dict:
    streams_of = jax.random.split(jax.random.key(seed), 8)
    return {
        "tokens": centred(streams_of[0], (TOKENS, D), 1.0, 6.0, ((0, 8),)),
        "w_in": centred(streams_of[1], (D, H * P_SIZE), D ** -0.5, 0.125, ((0, 8), (1, 4))),
        "b_in": centred(streams_of[2], (TOKENS, N), 0.088, 0.6, ((0, 8),), jnp.float32),
        "c_in": centred(streams_of[3], (TOKENS, N), 0.088, 0.6, ((0, 8),), jnp.float32),
        "dt": jnp.clip(jnp.exp(math.log(0.2) - 1.3862944 * jax.random.uniform(streams_of[4], (H, TOKENS), jnp.float32) ** shard_levels(streams_of[4], (H, TOKENS), ((0, 4), (1, 8)), -0.2, 0.2)), 0.05, 0.2),
        "log_rate": draw_log_rate(jax.random.fold_in(streams_of[7], 71), 0),
        "cot": centred(streams_of[6], (TOKENS, H * P_SIZE), 1.0, 6.0, ((0, 8), (1, 4))),
    }


HIGH = lax.Precision.HIGHEST
ascent = 0.05
rate_ascent = 0.5

def span_core(b_blk, c_blk, logdec):
    width = logdec.shape[1]
    cum = jnp.cumsum(logdec, axis=1)
    places = jnp.arange(width)
    lower = (places[:, None] >= places[None, :])[None]
    gap = cum[:, :, None] - cum[:, None, :]
    blend = jnp.where(lower, jnp.exp(jnp.where(lower, gap, 0.0)), 0.0)
    scores = jnp.dot(c_blk, b_blk.T, precision=HIGH)
    return (cum, gap, blend * scores[None])

def span_forward(x_blk, dt_blk, b_blk, cum, kern):
    kern_x = kern * dt_blk[:, None, :]
    y_local = jnp.einsum('hts,shp->thp', kern_x, x_blk, precision=HIGH)
    final = cum[:, -1]
    tail = (jnp.exp(final[:, None] - cum) * dt_blk).T
    state = jnp.einsum('sn,shp->hnp', b_blk, x_blk * tail[:, :, None], precision=HIGH)
    return (y_local, jnp.exp(final), state)

def span_entry(c_blk, cum, h_in):
    return jnp.einsum('tn,hnp->thp', c_blk, h_in, precision=HIGH) * jnp.exp(cum).T[:, :, None]

def span_lead(c_blk, cot_blk, cum):
    return jnp.einsum('tn,thp->hnp', c_blk, cot_blk * jnp.exp(cum).T[:, :, None], precision=HIGH)

def span_backward(x_blk, cot_blk, dt_blk, b_blk, cum, gap, kern, entry, h_in, after):
    final = cum[:, -1]
    kern_x = kern * dt_blk[:, None, :]
    back = jnp.einsum('hts,thp->shp', kern, cot_blk, precision=HIGH)
    fall = jnp.exp(final[:, None] - cum).T
    proj = jnp.einsum('sn,hnp->shp', b_blk, after, precision=HIGH)
    grad_x = dt_blk.T[:, :, None] * (back + fall[:, :, None] * proj)
    pairs = jnp.einsum('thp,shp->hts', cot_blk, x_blk, precision=HIGH)
    part = lax.optimization_barrier(jnp.sum(kern_x * gap * pairs, axis=(1, 2)))
    part = part + lax.optimization_barrier(jnp.sum(lax.optimization_barrier(jnp.sum(entry * cot_blk, axis=2)) * cum.T, axis=0))
    weight = fall * dt_blk.T * (final[:, None] - cum).T
    part = part + lax.optimization_barrier(jnp.sum(weight * lax.optimization_barrier(jnp.sum(proj * x_blk, axis=2)), axis=0))
    part = part + jnp.exp(final) * final * lax.optimization_barrier(jnp.sum(after * h_in, axis=(1, 2)))
    return (grad_x, part)

def reference(tokens, w_in, b_in, c_in, dt, log_rate, cot):
    blocks = TOKENS // Q
    x_bf = jnp.dot(tokens, w_in, preferred_element_type=jnp.float32).astype(jnp.bfloat16)
    x_all = x_bf.astype(jnp.float32).reshape(blocks, Q, H, P_SIZE)
    logdec = (-dt * jnp.exp(log_rate)[:, None]).reshape(H, blocks, Q).transpose(1, 0, 2)
    dt_all = dt.reshape(H, blocks, Q).transpose(1, 0, 2)
    b_all = b_in.astype(jnp.float32).reshape(blocks, Q, N)
    c_all = c_in.astype(jnp.float32).reshape(blocks, Q, N)
    cot_all = cot.astype(jnp.float32).reshape(blocks, Q, H, P_SIZE)
    zero_state = jnp.zeros((H, N, P_SIZE), jnp.float32)

    def forward(state_in, item):
        x_blk, dt_blk, l_blk, b_blk, c_blk = item
        cum, gap, kern = span_core(b_blk, c_blk, l_blk)
        y_local, decay, state = span_forward(x_blk, dt_blk, b_blk, cum, kern)
        y_blk = y_local + span_entry(c_blk, cum, state_in)
        return (decay[:, None, None] * state_in + state, (y_blk, state_in))
    _, (y_all, h_ins) = lax.scan(forward, zero_state, (x_all, dt_all, logdec, b_all, c_all))

    def backward(after, item):
        x_blk, cot_blk, dt_blk, l_blk, b_blk, c_blk, h_in = item
        cum, gap, kern = span_core(b_blk, c_blk, l_blk)
        entry = span_entry(c_blk, cum, h_in)
        grad_x, part = span_backward(x_blk, cot_blk, dt_blk, b_blk, cum, gap, kern, entry, h_in, after)
        lead = span_lead(c_blk, cot_blk, cum)
        return (jnp.exp(cum[:, -1])[:, None, None] * after + lead, (grad_x, part))
    _, (gx_all, parts) = lax.scan(backward, zero_state, (x_all, cot_all, dt_all, logdec, b_all, c_all, h_ins), reverse=True)
    gx_bf = gx_all.reshape(TOKENS, H * P_SIZE).astype(jnp.bfloat16)
    grad_w = jnp.dot(tokens.T, gx_bf, preferred_element_type=jnp.float32)
    grad_rate = lax.optimization_barrier(jnp.sum(parts, axis=0))
    rate_sq = jnp.sum(grad_rate * grad_rate)
    total = jnp.sum(grad_w * grad_w) + rate_sq
    scale = 1.0 / jnp.maximum(jnp.sqrt(total), 1.0)
    rate_scale = math.sqrt(H) / jnp.maximum(jnp.sqrt(rate_sq), 1.0)
    mixed = y_all.reshape(TOKENS, H * P_SIZE).astype(jnp.bfloat16)
    direction = grad_w * (math.sqrt(D * H * P_SIZE) * scale)
    perturbed = w_in.astype(jnp.float32) + ascent * scale * grad_w
    perturbed_rate = log_rate + rate_ascent * rate_scale * grad_rate
    return (mixed, direction, perturbed, perturbed_rate)
```

```python
import functools
import math

import jax
import jax.numpy as jnp
from jax import lax
from jax.experimental import pallas as pl
from jax.experimental.pallas import tpu as pltpu
from jax.sharding import PartitionSpec as P

P_SIZE = 64
LANES = 128
CHUNK = 256
MESH = pl.DeviceIdType.MESH
ascent = 0.05
rate_ascent = 0.5
F32 = jnp.float32
BF16 = jnp.bfloat16


def dot(a, b, ca=1, cb=0):
    return lax.dot_general(a, b, (((ca,), (cb,)), ((), ())), preferred_element_type=F32)


def split(a):
    high = a.astype(BF16)
    return high, (a - high.astype(F32)).astype(BF16)


def dot3(a, b, ca=1, cb=0):
    (ah, al), (bh, bl) = a, b
    return dot(ah, bh, ca, cb) + (dot(ah, bl, ca, cb) + dot(al, bh, ca, cb))


def loop(count, fn, start=0):
    def step(i, carry):
        fn(i)
        return carry

    lax.fori_loop(start, count, step, 0)


def mixer(
    n, nm, owners,
    tok, w, b, c, cot, lfull, dtfull, cumr, dtr,
    mixed, gw, rates,
    kern, scores, gx32, gxc, x_acc, x_bf, after, h_in,
    w_rx, tok_rx, gx_tx, gx_rx,
    dec_tx, dec_rx, lead_tx, lead_rx, after_tx, after_rx,
    st_tx, st_rx, h_tx, h_rx, pk_tx, pk_rx,
    w_s, w_r, tok_s, tok_r, gx_s, gx_r, dec_s, dec_r, lead_s, lead_r, af_s, af_r,
    st_s, st_r, h_s, h_r, pk_s, pk_r,
):
    me = lax.axis_index("seq")
    mm = lax.axis_index("mp")
    total = n * nm
    flat = me * nm + mm
    rows, width = cot.shape
    states = b.shape[1]
    pairs = width // LANES
    chunks = width // CHUNK
    piece = states // owners

    def copy(src, dst, ss, rs, peer):
        return pltpu.make_async_remote_copy(
            src_ref=src, dst_ref=dst, send_sem=ss, recv_sem=rs,
            device_id=(peer, mm), device_id_type=MESH,
        )

    def w_copy(peer, slot):
        return copy(w, w_rx.at[slot], w_s.at[peer], w_r.at[slot], peer)

    def tok_copy(peer, slot):
        return copy(tok.at[peer], tok_rx.at[slot], tok_s.at[peer], tok_r.at[slot], peer)

    def gx_copy(peer, slot):
        return copy(gx_tx, gx_rx.at[slot], gx_s.at[peer], gx_r.at[slot], peer)

    def dec_copy(peer, slot):
        return copy(dec_tx, dec_rx.at[slot], dec_s.at[peer], dec_r.at[slot], peer)

    def up_copy(tx, rx, ss, rs, peer, slot):
        return copy(tx.at[peer], rx.at[slot], ss.at[peer], rs.at[slot], peer)

    def pk_copy(peer_flat, slot):
        return pltpu.make_async_remote_copy(
            src_ref=pk_tx, dst_ref=pk_rx.at[slot], send_sem=pk_s.at[peer_flat],
            recv_sem=pk_r.at[slot], device_id=(peer_flat // nm, peer_flat % nm),
            device_id_type=MESH,
        )

    barrier = pltpu.get_barrier_semaphore()

    def greet(d):
        f = (flat + d) % total
        pl.semaphore_signal(barrier, inc=1, device_id=(f // nm, f % nm), device_id_type=MESH)

    loop(total, greet, 1)

    def chunk_ds(k):
        return pl.ds(pl.multiple_of(k * CHUNK, CHUNK), CHUNK)

    def pair_ds(k):
        return pl.ds(pl.multiple_of(k * LANES, LANES), LANES)

    def to_owner(tx, rx, ss, rs):
        def one(d):
            j = (me + d) % owners

            @pl.when(j != me)
            def _():
                up_copy(tx, rx, ss, rs, j, me).start()

            @pl.when(j == me)
            def _():
                rx[me] = tx[j]

        loop(owners, one)

    def owner_wait(tx, rx, ss, rs):
        def one(i):
            @pl.when(i != me)
            def _():
                up_copy(tx, rx, ss, rs, 0, i).wait_recv()

        loop(n, one)

    def from_owner(tx, rx, ss, rs):
        def one(d):
            j = (me + d) % n
            up_copy(tx, rx, ss, rs, j, me).start()

        rx[me] = tx[me]
        loop(n, one, 1)

    def from_owner_wait(tx, rx, ss, rs):
        def one(i):
            @pl.when(i != me)
            def _():
                up_copy(tx, rx, ss, rs, 0, i).wait_recv()

        loop(owners, one)

    def decay_row(j):
        d = dec_rx[j]
        return jnp.concatenate([d[k : k + 1, :] for k in range(pairs)], axis=1)

    final = lfull[rows - 1 : rows, :]
    dec = jnp.exp(final)
    for k in range(pairs):
        dec_tx[k : k + 1, :] = dec[:, k * LANES : (k + 1) * LANES]
    dec_rx[me] = dec_tx[...]
    b_val, c_val = b[...], c[...]
    b_split, c_split = split(b_val), split(c_val)
    bt_split, ct_split = split(b_val.T), split(c_val.T)

    def lead_chunk(k):
        ds = chunk_ds(k)
        lead = dot3(ct_split, split(cot[:, ds].astype(F32) * jnp.exp(lfull[:, ds])))
        for j in range(owners):
            lead_tx[j, :, ds] = lead[j * piece : (j + 1) * piece, :].astype(BF16)

    loop(chunks, lead_chunk)

    pl.semaphore_wait(barrier, total - 1)
    loop(n, lambda d: dec_copy((me + d) % n, me).start(), 1)
    to_owner(lead_tx, lead_rx, lead_s, lead_r)
    loop(n, lambda d: tok_copy((me + d) % n, me).start(), 1)

    scores[...] = dot3(c_split, b_split, 1, 1)
    lane = lax.broadcasted_iota(jnp.int32, (rows, LANES), 1)
    first = lane < P_SIZE

    def kern_pair(k):
        ds = pair_ds(k)
        level = lfull[:, ds]
        crow, drow = cumr[k], dtr[k]
        lower = lax.broadcasted_iota(jnp.int32, (rows, rows), 0) >= lax.broadcasted_iota(
            jnp.int32, (rows, rows), 1
        )
        cot_pair = cot[:, ds]
        parts = []
        for h in range(2):
            gap = level[:, h * P_SIZE : h * P_SIZE + 1] - crow[h : h + 1, :]
            blend = jnp.exp(jnp.where(lower, gap, -1e30))
            mat = (blend * (scores[...] * drow[h : h + 1, :])).astype(BF16)
            kern[2 * k + h] = mat
            parts.append(dot(mat, cot_pair, 0, 0))
        gx32[:, ds] = jnp.where(first, parts[0], parts[1])

    loop(pairs, kern_pair)

    loop(n, lambda d: dec_copy((me + d) % n, (me + n - d) % n).wait_recv(), 1)

    @pl.when(me < owners)
    def _():
        owner_wait(lead_tx, lead_rx, lead_s, lead_r)

        def step(i, acc):
            j = n - 1 - i
            after_tx[j] = acc.astype(BF16)
            return decay_row(j) * acc + lead_rx[j].astype(F32)

        lax.fori_loop(0, n, step, jnp.zeros((piece, width), F32))
        from_owner(after_tx, after_rx, af_s, af_r)

    loop(n, lambda d: w_copy((me + d) % n, me).start(), 1)
    from_owner_wait(after_tx, after_rx, af_s, af_r)
    for j in range(owners):
        after[j * piece : (j + 1) * piece, :] = after_rx[j]

    def gx_chunk(k):
        ds = chunk_ds(k)
        level = lfull[:, ds]
        a = after[:, ds]
        proj = dot(b_split[0], a) + dot(b_split[1], a)
        carry = dtfull[:, ds] * jnp.exp(level[rows - 1 : rows, :] - level) * proj
        gxc[:, ds] = carry
        whole = gx32[:, ds] + carry
        gx32[:, ds] = whole
        gx_tx[:, ds] = whole.astype(BF16)

    loop(chunks, gx_chunk)

    x_acc[...] = dot(tok[me], w[...], 0, 0)

    def project(d):
        src = (me + n - d) % n
        w_copy((me + d) % n, src).wait_recv()
        x_acc[...] += dot(tok[src], w_rx[src], 0, 0)

    loop(n, project, 1)

    def state_chunk(k):
        ds = chunk_ds(k)
        level = lfull[:, ds]
        x16 = x_acc[:, ds].astype(BF16)
        x_bf[:, ds] = x16
        tail = jnp.exp(level[rows - 1 : rows, :] - level) * dtfull[:, ds]
        state = dot3(bt_split, split(x16.astype(F32) * tail))
        for j in range(owners):
            st_tx[j, :, ds] = state[j * piece : (j + 1) * piece, :].astype(BF16)

    loop(chunks, state_chunk)
    to_owner(st_tx, st_rx, st_s, st_r)
    half = n // 2
    loop(half, lambda d: gx_copy((me + d) % n, me).start(), 1)

    def y_pair(k):
        ds = pair_ds(k)
        xp = x_bf[:, ds]
        x_acc[:, ds] = jnp.where(first, dot(kern[2 * k], xp), dot(kern[2 * k + 1], xp))

    loop(pairs, y_pair)

    @pl.when(me < owners)
    def _():
        owner_wait(st_tx, st_rx, st_s, st_r)

        def step(j, acc):
            h_tx[j] = acc.astype(BF16)
            return decay_row(j) * acc + st_rx[j].astype(F32)

        lax.fori_loop(0, n, step, jnp.zeros((piece, width), F32))
        from_owner(h_tx, h_rx, h_s, h_r)

    loop(n, lambda d: gx_copy((me + d) % n, me).start(), half)
    from_owner_wait(h_tx, h_rx, h_s, h_r)
    for j in range(owners):
        h_in[j * piece : (j + 1) * piece, :] = h_rx[j]

    pk_tx[...] = jnp.zeros(pk_tx.shape, F32)

    def out_chunk(k):
        ds = chunk_ds(k)
        level = lfull[:, ds]
        h = h_in[:, ds]
        y = x_acc[:, ds] + (dot(c_split[0], h) + dot(c_split[1], h)) * jnp.exp(level)
        mixed[:, ds] = y.astype(BF16)
        xs = x_bf[:, ds].astype(F32)
        last = level[rows - 1 : rows, :]
        inner = level * (y * cot[:, ds].astype(F32) - gx32[:, ds] * xs)
        part = jnp.sum(inner + last * (gxc[:, ds] * xs), axis=0, keepdims=True)
        cross = jnp.sum(after[:, ds].astype(F32) * h.astype(F32), axis=0, keepdims=True)
        part = part + jnp.exp(last) * last * cross
        for i in range(CHUNK // LANES):
            pk_tx[pl.ds(k * (CHUNK // LANES) + i, 1), :] = part[:, i * LANES : (i + 1) * LANES]

    loop(chunks, out_chunk)

    gw[...] = dot(tok[me], gx_tx[...])

    def weight(d):
        src = (me + n - d) % n
        tok_copy((me + d) % n, src).wait_recv()
        gx_copy((me + d) % n, src).wait_recv()
        gw[...] += dot(tok_rx[src], gx_rx[src])

    loop(n, weight, 1)
    square = jnp.zeros((1, LANES), F32)
    for k in range(pairs):
        g = gw[:, k * LANES : (k + 1) * LANES]
        square = square + jnp.sum(g * g, axis=0, keepdims=True)
    pk_tx[pairs : pairs + 1, :] = square
    pk_rx[flat] = pk_tx[...]
    loop(total, lambda d: pk_copy((flat + d) % total, flat).start(), 1)

    def sent(d):
        peer = (me + d) % n
        w_copy(peer, me).wait_send()
        tok_copy(peer, me).wait_send()
        gx_copy(peer, me).wait_send()
        dec_copy(peer, me).wait_send()

    loop(n, sent, 1)

    def sent_up(j):
        @pl.when(j != me)
        def _():
            up_copy(lead_tx, lead_rx, lead_s, lead_r, j, me).wait_send()
            up_copy(st_tx, st_rx, st_s, st_r, j, me).wait_send()

    loop(owners, sent_up)

    @pl.when(me < owners)
    def _():
        def sent_down(d):
            j = (me + d) % n
            up_copy(after_tx, after_rx, af_s, af_r, j, me).wait_send()
            up_copy(h_tx, h_rx, h_s, h_r, j, me).wait_send()

        loop(n, sent_down, 1)

    loop(total, lambda d: pk_copy((flat + d) % total, (flat + total - d) % total).wait_recv(), 1)
    for m in range(nm):
        acc = lax.fori_loop(
            0, n, lambda s, a: a + pk_rx[s * nm + m], jnp.zeros(pk_tx.shape, F32)
        )
        rates[m] = acc
    loop(total, lambda d: pk_copy((flat + d) % total, flat).wait_send(), 1)


def body(n, nm, tokens, w_in, b_in, c_in, dt, log_rate, cot):
    rows, model = tokens.shape
    depth, width = w_in.shape
    heads = dt.shape[0]
    states = b_in.shape[1]
    pairs = width // LANES
    owners = min(n, states // 16)
    piece = states // owners
    total = n * nm
    packet = (pairs + 8) // 8 * 8
    cum = jnp.cumsum(-dt * jnp.exp(log_rate)[:, None], axis=1)
    lfull = jnp.repeat(cum.T, P_SIZE, axis=1)
    dtfull = jnp.repeat(dt.T, P_SIZE, axis=1)
    tok = tokens.T.reshape(n, depth, rows)
    dma = pltpu.SemaphoreType.DMA
    vm = pltpu.VMEM
    scratch = [
        vm((heads, rows, rows), BF16),
        vm((rows, rows), F32),
        vm((rows, width), F32),
        vm((rows, width), F32),
        vm((rows, width), F32),
        vm((rows, width), BF16),
        vm((states, width), BF16),
        vm((states, width), BF16),
        vm((n, depth, width), BF16),
        vm((n, depth, rows), BF16),
        vm((rows, width), BF16),
        vm((n, rows, width), BF16),
        vm((pairs, LANES), F32),
        vm((n, pairs, LANES), F32),
        vm((owners, piece, width), BF16),
        vm((n, piece, width), BF16),
        vm((n, piece, width), BF16),
        vm((owners, piece, width), BF16),
        vm((owners, piece, width), BF16),
        vm((n, piece, width), BF16),
        vm((n, piece, width), BF16),
        vm((owners, piece, width), BF16),
        vm((packet, LANES), F32),
        vm((total, packet, LANES), F32),
    ] + [dma((n,))] * 16 + [dma((total,))] * 2
    spec = pl.BlockSpec(memory_space=pltpu.VMEM)
    mixed, grad_w, rates = pl.pallas_call(
        functools.partial(mixer, n, nm, owners),
        out_shape=(
            jax.ShapeDtypeStruct((rows, width), BF16),
            jax.ShapeDtypeStruct((depth, width), F32),
            jax.ShapeDtypeStruct((nm, packet, LANES), F32),
        ),
        in_specs=[spec] * 9,
        out_specs=(spec,) * 3,
        scratch_shapes=scratch,
        compiler_params=pltpu.CompilerParams(
            collective_id=0, has_side_effects=True, vmem_limit_bytes=67_000_000
        ),
    )(
        tok, w_in, b_in, c_in, cot, lfull, dtfull,
        cum.reshape(pairs, 2, rows), dt.reshape(pairs, 2, rows),
    )
    by_head = jnp.sum(rates[:, :pairs].reshape(nm, heads, P_SIZE), axis=2)
    rate_sq = jnp.sum(by_head * by_head)
    total_sq = jnp.sum(rates[:, pairs]) + rate_sq
    grad_rate = lax.dynamic_index_in_dim(by_head, lax.axis_index("mp"), 0, False)
    scale = 1.0 / jnp.maximum(jnp.sqrt(total_sq), 1.0)
    rate_scale = math.sqrt(heads * nm) / jnp.maximum(jnp.sqrt(rate_sq), 1.0)
    direction = grad_w * (math.sqrt(model * width * nm) * scale)
    perturbed = w_in.astype(F32) + ascent * scale * grad_w
    perturbed_rate = log_rate + rate_ascent * rate_scale * grad_rate
    return (mixed, direction, perturbed, perturbed_rate)


def solution(mesh):
    in_specs = (
        P("seq", None), P("seq", "mp"), P("seq", None), P("seq", None),
        P("mp", "seq"), P("mp"), P("seq", "mp"),
    )
    out_specs = (P("seq", "mp"), P("seq", "mp"), P("seq", "mp"), P("mp"))
    return jax.shard_map(
        functools.partial(body, mesh.shape["seq"], mesh.shape["mp"]),
        mesh=mesh, in_specs=in_specs, out_specs=out_specs, check_vma=False,
    )
```
